32 devices in a mesh: tm: 8 (over y, x, core), space: 4 (over z).
Axes of the slice: x: 2, y: 2, z: 4, core: 2. Of those that a mesh axis runs over, the one named last changes fastest.
Arguments:
- evecs: float32 [8, 2, 3072, 256], P('tm', None, 'space'), may hold values from -0.109375 to 0.109375
- solutions: float32 [8, 2, 3072, 128], P('tm', None, 'space'), may hold values from -6 to 6
- sink_time_weight: float32 [8, 8], P(None, 'tm'), may hold values from 0.1 to 1
- noise_source_vector: float32 [8, 2, 4, 256], P('tm'), may hold values from -6 to 6
- probe: float32 [8, 2, 4, 256], P('tm'), may hold values from -6 to 6
- dilution_spin_index: int32 [8, 4], P('tm'), may hold values from 0 to 3
- dilution_lace_index: int32 [8, 4], P('tm'), may hold values from 0 to 7
Outputs:
- smeared: float32 [8, 2, 16, 3072], P('tm', None, None, 'space')
The draws below stay inside these ranges and needn't reach their ends.
All inputs are finite; a program needn't handle non-finite values.
Results may differ from the reference program's by a relative error of at most 0.000071.
Values sent between devices are 32-bit elements; how exact they have to be, the bound alone decides.
No kernel may reach another device: no remote copies, remote signals or barrier semaphores. Data moves between devices by JAX's collectives and lax.ppermute only.
A program may use at most 64 MiB of HBM per device.

```python
import math
import jax
import jax.numpy as jnp
from jax import lax

EIGEN_COUNT = 256
DILUTION_COUNT = 4
SPIN_COUNT = 4
LACE_CLASSES = 8
TIME_SLICES = 8
ROWS = 3072
COLS = 128


def plant(drawn, key, low, high):
    index_at = [jax.random.randint(jax.random.fold_in(key, axis), (), 0, length) for axis, length in enumerate(drawn.shape)]
    main_axis = drawn.shape.index(max(drawn.shape))
    next_to = index_at[:main_axis] + [(index_at[main_axis] + 1) % drawn.shape[main_axis]] + index_at[main_axis + 1:]
    return drawn.at[tuple(index_at)].set(low).at[tuple(next_to)].set(high)


def shard_levels(rng, dims, cuts, low, top_value):
    loudness, own = 1.0, jax.random.fold_in(rng, 6)
    for position, shards_of in cuts:
        draws = jnp.exp(jax.random.uniform(jax.random.fold_in(own, position), (shards_of,), jnp.float32, low / len(cuts), top_value / len(cuts)))
        loudness = loudness * jnp.repeat(draws, dims[position] // shards_of).reshape([-1 if axis == position else 1 for axis in range(len(dims))])
    return loudness


def centred(stream_key, extent, deviation, limit, cuts=(), held_as=jnp.bfloat16):
    level = shard_levels(stream_key, extent, cuts, -0.22, 0.18) if cuts else 1.0
    values = jax.random.normal(stream_key, extent, jnp.float32) * deviation * level
    return jnp.minimum(jnp.maximum(values, -limit), limit).astype(held_as)


def setup_inputs(seed: int = 0) -> dict:
    key_list = jax.random.split(jax.random.key(seed), 8)
    return {
        "evecs": centred(key_list[0], (TIME_SLICES, 2, ROWS, EIGEN_COUNT), ROWS ** -0.5, 0.109375, ((0, 8), (2, 4)), jnp.float32),
        "solutions": centred(key_list[1], (TIME_SLICES, 2, ROWS, COLS), 1.0, 6.0, ((0, 8), (2, 4)), jnp.float32),
        "sink_time_weight": jnp.clip(jnp.exp(math.log(1.0) - 2.3025851 * jax.random.uniform(key_list[2], (TIME_SLICES, TIME_SLICES), jnp.float32) ** shard_levels(key_list[2], (TIME_SLICES, TIME_SLICES), ((1, 8),), -0.2, 0.2)), 0.1, 1.0),
        "noise_source_vector": centred(key_list[3], (TIME_SLICES, 2, SPIN_COUNT, EIGEN_COUNT), 1.0, 6.0, ((0, 8),), jnp.float32),
        "probe": centred(key_list[4], (TIME_SLICES, 2, SPIN_COUNT, EIGEN_COUNT), 1.0, 6.0, ((0, 8),), jnp.float32),
        "dilution_spin_index": plant(jax.random.randint(key_list[5], (TIME_SLICES, DILUTION_COUNT), 0, SPIN_COUNT), jax.random.fold_in(key_list[5], 1), 0, SPIN_COUNT - 1).astype(jnp.int32),
        "dilution_lace_index": plant(jax.random.randint(key_list[6], (TIME_SLICES, DILUTION_COUNT), 0, LACE_CLASSES), jax.random.fold_in(key_list[6], 1), 0, LACE_CLASSES - 1).astype(jnp.int32),
    }


def project(pieces):
    vreal, vimag, preal, pimag = pieces
    hp = lax.Precision.HIGHEST
    real = jnp.dot(vreal.T, preal, precision=hp, preferred_element_type=jnp.float32) + jnp.dot(vimag.T, pimag, precision=hp, preferred_element_type=jnp.float32)
    imag = jnp.dot(vreal.T, pimag, precision=hp, preferred_element_type=jnp.float32) - jnp.dot(vimag.T, preal, precision=hp, preferred_element_type=jnp.float32)
    return jnp.stack([real, imag])


def reference(evecs, solutions, sink_time_weight, noise_source_vector, probe, dilution_spin_index, dilution_lace_index):
    hp = lax.Precision.HIGHEST
    mode_coefficients = lax.map(project, (evecs[:, 0], evecs[:, 1], solutions[:, 0], solutions[:, 1]))
    mode_coefficients = mode_coefficients.reshape(TIME_SLICES, 2, EIGEN_COUNT, TIME_SLICES, DILUTION_COUNT * SPIN_COUNT)
    summed_result = jnp.einsum("tcnuj,tu->ucnj", mode_coefficients, sink_time_weight, precision=hp)
    summed_result = summed_result.reshape(TIME_SLICES, 2, EIGEN_COUNT, DILUTION_COUNT, SPIN_COUNT)
    vector_lanes = jnp.arange(EIGEN_COUNT, dtype=jnp.int32) % LACE_CLASSES
    lace_matches = (vector_lanes[None, None, :] == dilution_lace_index[:, :, None]).astype(jnp.float32)
    spin_matches = (jnp.arange(SPIN_COUNT, dtype=jnp.int32)[None, None, :] == dilution_spin_index[:, :, None]).astype(jnp.float32)
    ereal, eimag = noise_source_vector[:, 0], noise_source_vector[:, 1]
    preal, pimag = probe[:, 0], probe[:, 1]
    prod_real = ereal * preal + eimag * pimag
    prod_imag = ereal * pimag - eimag * preal
    w_real = jnp.einsum("tkm,tsm->tks", lace_matches, prod_real, precision=hp) * spin_matches
    w_imag = jnp.einsum("tkm,tsm->tks", lace_matches, prod_imag, precision=hp) * spin_matches
    y_real, y_imag = summed_result[:, 0], summed_result[:, 1]
    z_real = jnp.einsum("tnka,tks->tnas", y_real, w_real, precision=hp) - jnp.einsum("tnka,tks->tnas", y_imag, w_imag, precision=hp)
    z_imag = jnp.einsum("tnka,tks->tnas", y_real, w_imag, precision=hp) + jnp.einsum("tnka,tks->tnas", y_imag, w_real, precision=hp)
    z_real = z_real.reshape(TIME_SLICES, EIGEN_COUNT, SPIN_COUNT * SPIN_COUNT)
    z_imag = z_imag.reshape(TIME_SLICES, EIGEN_COUNT, SPIN_COUNT * SPIN_COUNT)
    vreal, vimag = evecs[:, 0], evecs[:, 1]
    f_real = jnp.einsum("trn,tnq->tqr", vreal, z_real, precision=hp) - jnp.einsum("trn,tnq->tqr", vimag, z_imag, precision=hp)
    f_imag = jnp.einsum("trn,tnq->tqr", vreal, z_imag, precision=hp) + jnp.einsum("trn,tnq->tqr", vimag, z_real, precision=hp)
    return jnp.stack([f_real, f_imag], axis=1)
```

```python
import functools

import jax
import jax.numpy as jnp
from jax import lax
from jax.experimental import pallas as pl
from jax.experimental.pallas import tpu as pltpu
from jax.sharding import PartitionSpec as P

LACE_CLASSES = 8
SPIN_COUNT = 4
BF16 = jnp.bfloat16
F32 = jnp.float32
VMEM_SPEC = pl.BlockSpec(memory_space=pltpu.VMEM)
SMEM_SPEC = pl.BlockSpec(memory_space=pltpu.SMEM)


def split(x):
    high = x.astype(BF16)
    low = (x - high.astype(F32)).astype(BF16)
    return high, low


def dot3(left, right, contract=((1,), (0,))):
    lh, ll = left
    rh, rl = right
    mul = functools.partial(
        lax.dot_general, dimension_numbers=(contract, ((), ())), preferred_element_type=F32
    )
    rows = lh.shape[0]
    both = mul(jnp.concatenate([lh, ll], 0), rh)
    return both[:rows] + both[rows:] + mul(lh, rl)


def project_kernel(chips, index_ref, evecs_ref, solutions_ref, keep_ref, send_ref, total_ref):
    step = pl.program_id(0)
    rows, modes = evecs_ref.shape[2:]
    cols = solutions_ref.shape[3]
    half = cols // (2 * chips)
    real = solutions_ref[0, 0].T
    imag = solutions_ref[0, 1].T
    left = jnp.concatenate(
        [jnp.concatenate([real, imag], 0), jnp.concatenate([imag, -real], 0)], 1
    )
    right = evecs_ref[0].reshape(2 * rows, modes)
    value = dot3(split(left), split(right))

    @pl.when(step == 0)
    def _():
        total_ref[...] = value

    @pl.when(step > 0)
    def _():
        total_ref[...] += value

    @pl.when(step == pl.num_programs(0) - 1)
    def _():
        for out, base in ((keep_ref, 0), (send_ref, chips)):
            for m in range(chips):
                block = index_ref[base + m]
                for part in range(2):
                    start = pl.multiple_of(part * cols + block * half, 8)
                    out[m, part * half : (part + 1) * half] = total_ref[pl.ds(start, half)]


def project(evecs, solutions, blocks, chips):
    rows, modes = evecs.shape[2:]
    cols = solutions.shape[3]
    block_rows = 2 * cols // (2 * chips)
    step = 256 if rows % 256 == 0 else rows
    out = jax.ShapeDtypeStruct((chips, block_rows, modes), F32)
    whole = pl.BlockSpec((chips, block_rows, modes), lambda i, s: (0, 0, 0))
    return pl.pallas_call(
        functools.partial(project_kernel, chips),
        grid_spec=pltpu.PrefetchScalarGridSpec(
            num_scalar_prefetch=1,
            grid=(rows // step,),
            in_specs=[
                pl.BlockSpec((1, 2, step, modes), lambda i, s: (0, 0, i, 0)),
                pl.BlockSpec((1, 2, step, cols), lambda i, s: (0, 0, i, 0)),
            ],
            out_specs=[whole, whole],
            scratch_shapes=[pltpu.VMEM((2 * cols, modes), F32)],
        ),
        out_shape=[out, out],
        name="project",
    )(blocks, evecs, solutions)


def mixing_matrix(noise_ref, probe_ref, spin_ref, lace_ref, width):
    noise_real, noise_imag = noise_ref[0, 0], noise_ref[0, 1]
    probe_real, probe_imag = probe_ref[0, 0], probe_ref[0, 1]
    prod_real = noise_real * probe_real + noise_imag * probe_imag
    prod_imag = noise_real * probe_imag - noise_imag * probe_real
    spins, modes = prod_real.shape
    groups = width // spins
    prod = jnp.concatenate([prod_real] * groups + [prod_imag] * groups, 0)
    lanes = lax.broadcasted_iota(jnp.int32, (2 * width, modes), 1) % LACE_CLASSES
    row = lax.broadcasted_iota(jnp.int32, (2 * width, width), 0) % width
    col = lax.broadcasted_iota(jnp.int32, (2 * width, width), 1)
    same = (row // spins) == (col % groups)
    both = jnp.zeros((2 * width, width), F32)
    for k in range(width // groups):
        picked = jnp.sum(jnp.where(lanes == lace_ref[0, k], prod, 0.0), axis=1, keepdims=True)
        on = same & ((col // groups) == k) & ((row % spins) == spin_ref[0, k])
        both = both + jnp.where(on, picked, 0.0)
    real, imag = both[:width], both[width:]
    return jnp.concatenate(
        [jnp.concatenate([real, -imag], 1), jnp.concatenate([imag, real], 1)], 0
    )


def recombine_kernel(copies, masks, me_ref, weight_ref, noise_ref, probe_ref, spin_ref, lace_ref, *refs):
    keep_ref, recv_ref = refs[:2]
    others, out_ref = refs[2:-1], refs[-1]
    me = me_ref[0]
    total = keep_ref[0] * weight_ref[me, 0] + recv_ref[0] * weight_ref[me ^ 1, 0]
    for mask, ref in zip(masks, others):
        total += ref[0] * weight_ref[me ^ mask, 0] + ref[1] * weight_ref[me ^ mask ^ 1, 0]
    mix = mixing_matrix(noise_ref, probe_ref, spin_ref, lace_ref, total.shape[0] // 2)
    value = dot3(split(mix), split(total))
    for i in range(copies):
        out_ref[i] = value


def smear_kernel(evecs_ref, parts_ref, out_ref):
    total = parts_ref[0]
    for i in range(1, parts_ref.shape[0]):
        total += parts_ref[i]
    width = total.shape[0] // 2
    turned = jnp.concatenate([-total[width:], total[:width]], 0)
    value = dot3(split(total), split(evecs_ref[0, 0]), ((1,), (1,)))
    value += dot3(split(turned), split(evecs_ref[0, 1]), ((1,), (1,)))
    out_ref[0, 0] = value[:width]
    out_ref[0, 1] = value[width:]


def per_device(
    evecs,
    solutions,
    sink_time_weight,
    noise_source_vector,
    probe,
    dilution_spin_index,
    dilution_lace_index,
):
    n_time, n_space = lax.axis_size("tm"), lax.axis_size("space")
    rows, modes = evecs.shape[2:]
    width = solutions.shape[3] // n_time
    chips = n_time // 2
    me = lax.axis_index("tm").astype(jnp.int32)
    masks = [2 * m + bin(m).count("1") % 2 for m in range(chips)]
    blocks = me ^ jnp.array(masks + [mask ^ 1 for mask in masks], jnp.int32)
    keep, send = project(evecs, solutions, blocks, chips)

    def swap(value, mask):
        return lax.ppermute(value, "tm", [(i, i ^ mask) for i in range(n_time)])

    recv = swap(send, 1)
    pairs = [jnp.stack([keep[m], recv[m]]) for m in range(1, chips)]
    others = [swap(pair, mask) for pair, mask in zip(pairs, masks[1:])]
    block = (2 * width, modes)
    parts = pl.pallas_call(
        functools.partial(recombine_kernel, n_space, masks[1:]),
        in_specs=[SMEM_SPEC, SMEM_SPEC, VMEM_SPEC, VMEM_SPEC, SMEM_SPEC, SMEM_SPEC]
        + [VMEM_SPEC] * (chips + 1),
        out_specs=VMEM_SPEC,
        out_shape=jax.ShapeDtypeStruct((n_space,) + block, F32),
        name="recombine",
    )(
        me[None],
        sink_time_weight,
        noise_source_vector,
        probe,
        dilution_spin_index,
        dilution_lace_index,
        keep[:1],
        recv[:1],
        *others,
    )
    parts = lax.all_to_all(parts, "space", 0, 0, tiled=True)
    return pl.pallas_call(
        smear_kernel,
        in_specs=[VMEM_SPEC, VMEM_SPEC],
        out_specs=VMEM_SPEC,
        out_shape=jax.ShapeDtypeStruct((1, 2, width, rows), F32),
        name="smear",
    )(evecs, parts)


def solution(mesh):
    placed = (
        P("tm", None, "space", None),
        P("tm", None, "space", None),
        P(None, "tm"),
        P("tm", None, None, None),
        P("tm", None, None, None),
        P("tm", None),
        P("tm", None),
    )
    return jax.shard_map(
        per_device,
        mesh=mesh,
        in_specs=placed,
        out_specs=P("tm", None, None, "space"),
        check_vma=False,
    )
```

```python
import functools

import jax
import jax.numpy as jnp
from jax import lax
from jax.experimental import pallas as pl
from jax.experimental.pallas import tpu as pltpu
from jax.sharding import PartitionSpec as P

LACE_CLASSES = 8
SPIN_COUNT = 4
BF16 = jnp.bfloat16
F32 = jnp.float32
VMEM_SPEC = pl.BlockSpec(memory_space=pltpu.VMEM)
SMEM_SPEC = pl.BlockSpec(memory_space=pltpu.SMEM)


def split(x):
    high = x.astype(BF16)
    low = (x - high.astype(F32)).astype(BF16)
    return high, low


def dot3(left, right, contract=((1,), (0,))):
    lh, ll = left
    rh, rl = right
    mul = functools.partial(
        lax.dot_general, dimension_numbers=(contract, ((), ())), preferred_element_type=F32
    )
    rows = lh.shape[0]
    both = mul(jnp.concatenate([lh, ll], 0), rh)
    return both[:rows] + both[rows:] + mul(lh, rl)


def project_kernel(masks, evecs_ref, solutions_ref, keep_ref, send_ref, total_ref):
    step = pl.program_id(0)
    chips = len(masks)
    me = lax.axis_index("tm").astype(jnp.int32)
    rows, modes = evecs_ref.shape[2:]
    cols = solutions_ref.shape[3]
    half = cols // (2 * chips)
    real = solutions_ref[0, 0].T
    imag = solutions_ref[0, 1].T
    left = jnp.concatenate(
        [jnp.concatenate([real, imag], 0), jnp.concatenate([imag, -real], 0)], 1
    )
    right = evecs_ref[0].reshape(2 * rows, modes)
    value = dot3(split(left), split(right))

    @pl.when(step == 0)
    def _():
        total_ref[...] = value

    @pl.when(step > 0)
    def _():
        total_ref[...] += value

    @pl.when(step == pl.num_programs(0) - 1)
    def _():
        for out, core in ((keep_ref, 0), (send_ref, 1)):
            for m, mask in enumerate(masks):
                block = me ^ (mask ^ core)
                for part in range(2):
                    start = pl.multiple_of(part * cols + block * half, 8)
                    out[m, part * half : (part + 1) * half] = total_ref[pl.ds(start, half)]


def project(evecs, solutions, masks):
    chips = len(masks)
    rows, modes = evecs.shape[2:]
    cols = solutions.shape[3]
    block_rows = 2 * cols // (2 * chips)
    step = 256 if rows % 256 == 0 else rows
    out = jax.ShapeDtypeStruct((chips, block_rows, modes), F32)
    whole = pl.BlockSpec((chips, block_rows, modes), lambda i: (0, 0, 0))
    return pl.pallas_call(
        functools.partial(project_kernel, masks),
        grid=(rows // step,),
        in_specs=[
            pl.BlockSpec((1, 2, step, modes), lambda i: (0, 0, i, 0)),
            pl.BlockSpec((1, 2, step, cols), lambda i: (0, 0, i, 0)),
        ],
        out_specs=[whole, whole],
        scratch_shapes=[pltpu.VMEM((2 * cols, modes), F32)],
        out_shape=[out, out],
        compiler_params=pltpu.CompilerParams(vmem_limit_bytes=32 << 20),
        name="project",
    )(evecs, solutions)


def mixing_matrix(noise_ref, probe_ref, spin_ref, lace_ref, width):
    noise_real, noise_imag = noise_ref[0, 0], noise_ref[0, 1]
    probe_real, probe_imag = probe_ref[0, 0], probe_ref[0, 1]
    prod_real = noise_real * probe_real + noise_imag * probe_imag
    prod_imag = noise_real * probe_imag - noise_imag * probe_real
    spins, modes = prod_real.shape
    groups = width // spins
    prod = jnp.concatenate([prod_real] * groups + [prod_imag] * groups, 0)
    lanes = lax.broadcasted_iota(jnp.int32, (2 * width, modes), 1) % LACE_CLASSES
    row = lax.broadcasted_iota(jnp.int32, (2 * width, width), 0) % width
    col = lax.broadcasted_iota(jnp.int32, (2 * width, width), 1)
    same = (row // spins) == (col % groups)
    both = jnp.zeros((2 * width, width), F32)
    for k in range(width // groups):
        picked = jnp.sum(jnp.where(lanes == lace_ref[0, k], prod, 0.0), axis=1, keepdims=True)
        on = same & ((col // groups) == k) & ((row % spins) == spin_ref[0, k])
        both = both + jnp.where(on, picked, 0.0)
    real, imag = both[:width], both[width:]
    return jnp.concatenate(
        [jnp.concatenate([real, -imag], 1), jnp.concatenate([imag, real], 1)], 0
    )


def recombine_kernel(masks, weight_ref, noise_ref, probe_ref, spin_ref, lace_ref, *refs):
    keep_ref, recv_ref = refs[:2]
    others, out_ref = refs[2:-1], refs[-1]
    me = lax.axis_index("tm").astype(jnp.int32)
    total = keep_ref[0] * weight_ref[0, me] + recv_ref[0] * weight_ref[0, me ^ 1]
    for mask, ref in zip(masks, others):
        total += ref[0] * weight_ref[0, me ^ mask] + ref[1] * weight_ref[0, me ^ mask ^ 1]
    mix = mixing_matrix(noise_ref, probe_ref, spin_ref, lace_ref, total.shape[0] // 2)
    out_ref[...] = dot3(split(mix), split(total))


def smear_kernel(evecs_ref, part_ref, *refs):
    out_ref = refs[-1]
    total = part_ref[...]
    for ref in refs[:-1]:
        total += ref[...]
    width = total.shape[0] // 2
    turned = jnp.concatenate([-total[width:], total[:width]], 0)
    value = dot3(split(total), split(evecs_ref[0, 0]), ((1,), (1,)))
    value += dot3(split(turned), split(evecs_ref[0, 1]), ((1,), (1,)))
    out_ref[0, 0] = value[:width]
    out_ref[0, 1] = value[width:]


def per_device(
    evecs,
    solutions,
    sink_time_weight,
    noise_source_vector,
    probe,
    dilution_spin_index,
    dilution_lace_index,
):
    n_time, n_space = lax.axis_size("tm"), lax.axis_size("space")
    rows, modes = evecs.shape[2:]
    width = solutions.shape[3] // n_time
    chips = n_time // 2
    masks = [2 * m + bin(m).count("1") % 2 for m in range(chips)]
    keep, send = project(evecs, solutions, masks)

    def swap(value, axis, mask):
        size = lax.axis_size(axis)
        return lax.ppermute(value, axis, [(i, i ^ mask) for i in range(size)])

    recv = swap(send, "tm", 1)
    pairs = [jnp.stack([keep[m], recv[m]]) for m in range(1, chips)]
    others = [swap(pair, "tm", mask) for pair, mask in zip(pairs, masks[1:])]
    part = pl.pallas_call(
        functools.partial(recombine_kernel, masks[1:]),
        in_specs=[SMEM_SPEC, VMEM_SPEC, VMEM_SPEC, SMEM_SPEC, SMEM_SPEC]
        + [VMEM_SPEC] * (chips + 1),
        out_specs=VMEM_SPEC,
        out_shape=jax.ShapeDtypeStruct((2 * width, modes), F32),
        compiler_params=pltpu.CompilerParams(vmem_limit_bytes=8 << 20),
        name="recombine",
    )(
        sink_time_weight.T,
        noise_source_vector,
        probe,
        dilution_spin_index,
        dilution_lace_index,
        keep[:1],
        recv[:1],
        *others,
    )
    parts = [swap(part, "space", mask) for mask in range(1, n_space)]
    return pl.pallas_call(
        smear_kernel,
        in_specs=[VMEM_SPEC] * (n_space + 1),
        out_specs=VMEM_SPEC,
        out_shape=jax.ShapeDtypeStruct((1, 2, width, rows), F32),
        compiler_params=pltpu.CompilerParams(vmem_limit_bytes=16 << 20),
        name="smear",
    )(evecs, part, *parts)


def solution(mesh):
    placed = (
        P("tm", None, "space", None),
        P("tm", None, "space", None),
        P(None, "tm"),
        P("tm", None, None, None),
        P("tm", None, None, None),
        P("tm", None),
        P("tm", None),
    )
    return jax.shard_map(
        per_device,
        mesh=mesh,
        in_specs=placed,
        out_specs=P("tm", None, None, "space"),
        check_vma=False,
    )
```

```python
import functools

import jax
import jax.numpy as jnp
from jax import lax
from jax.experimental import pallas as pl
from jax.experimental.pallas import tpu as pltpu
from jax.sharding import PartitionSpec as P

LACE_CLASSES = 8
STEP = 256
BF16 = jnp.bfloat16
F32 = jnp.float32
VMEM_SPEC = pl.BlockSpec(memory_space=pltpu.VMEM)
SMEM_SPEC = pl.BlockSpec(memory_space=pltpu.SMEM)


def split(x):
    high = x.astype(BF16)
    low = (x - high.astype(F32)).astype(BF16)
    return high, low


def dot3(left, right, contract=((1,), (0,))):
    lh, ll = left
    rh, rl = right
    mul = functools.partial(
        lax.dot_general, dimension_numbers=(contract, ((), ())), preferred_element_type=F32
    )
    rows = lh.shape[0]
    both = mul(jnp.concatenate([lh, ll], 0), rh)
    return both[:rows] + both[rows:] + mul(lh, rl)


def project_kernel(
    masks, evecs_hbm, solutions_hbm, keep_ref, send_ref, high_ref, low_ref, evecs_ref, solutions_ref, total_ref, sems
):
    chunks, _, step, modes = evecs_ref.shape
    cols = solutions_ref.shape[3]
    half = cols // (2 * len(masks))
    copies = []
    for i in range(chunks):
        rows = pl.ds(i * step, step)
        pair = (
            pltpu.make_async_copy(solutions_hbm.at[0, :, rows], solutions_ref.at[i], sems.at[0, i]),
            pltpu.make_async_copy(evecs_hbm.at[0, :, rows], evecs_ref.at[i], sems.at[1, i]),
        )
        for copy in pair:
            copy.start()
        copies.append(pair)
    for i in range(chunks):
        copies[i][0].wait()
        real = solutions_ref[i, 0].T
        imag = solutions_ref[i, 1].T
        left = split(
            jnp.concatenate(
                [jnp.concatenate([real, imag], 0), jnp.concatenate([imag, -real], 0)], 1
            )
        )
        copies[i][1].wait()
        right = split(evecs_ref[i].reshape(2 * step, modes))
        for ref, value in zip((high_ref, low_ref), right):
            for part in range(2):
                ref[part, i * step : (i + 1) * step] = value[part * step : (part + 1) * step]
        value = dot3(left, right)
        if i == 0:
            total_ref[...] = value
        else:
            total_ref[...] += value
    me = lax.axis_index("tm").astype(jnp.int32)
    for out, core in ((keep_ref, 1), (send_ref, 0)):
        for m, mask in enumerate(masks):
            block = me ^ (mask ^ core)
            for part in range(2):
                start = pl.multiple_of(part * cols + block * half, 8)
                out[m, part * half : (part + 1) * half] = total_ref[pl.ds(start, half)]


def project(evecs, solutions, masks):
    chips = len(masks)
    rows, modes = evecs.shape[2:]
    cols = solutions.shape[3]
    block_rows = 2 * cols // (2 * chips)
    step = STEP if rows % STEP == 0 else rows
    chunks = rows // step
    out = jax.ShapeDtypeStruct((chips, block_rows, modes), F32)
    held = jax.ShapeDtypeStruct((2, rows, modes), BF16)
    return pl.pallas_call(
        functools.partial(project_kernel, masks),
        in_specs=[pl.BlockSpec(memory_space=pltpu.HBM)] * 2,
        out_specs=[VMEM_SPEC] * 4,
        scratch_shapes=[
            pltpu.VMEM((chunks, 2, step, modes), F32),
            pltpu.VMEM((chunks, 2, step, cols), F32),
            pltpu.VMEM((2 * cols, modes), F32),
            pltpu.SemaphoreType.DMA((2, chunks)),
        ],
        out_shape=[out, out, held, held],
        compiler_params=pltpu.CompilerParams(vmem_limit_bytes=54_000_000),
        name="project",
    )(evecs, solutions)


def mixing_matrix(noise_ref, probe_ref, spin_ref, lace_ref, width):
    noise_real, noise_imag = noise_ref[0, 0], noise_ref[0, 1]
    probe_real, probe_imag = probe_ref[0, 0], probe_ref[0, 1]
    prod_real = noise_real * probe_real + noise_imag * probe_imag
    prod_imag = noise_real * probe_imag - noise_imag * probe_real
    spins, modes = prod_real.shape
    groups = width // spins
    prod = jnp.concatenate([prod_real] * groups + [prod_imag] * groups, 0)
    lanes = lax.broadcasted_iota(jnp.int32, (2 * width, modes), 1) % LACE_CLASSES
    row = lax.broadcasted_iota(jnp.int32, (2 * width, width), 0) % width
    col = lax.broadcasted_iota(jnp.int32, (2 * width, width), 1)
    same = (row // spins) == (col % groups)
    both = jnp.zeros((2 * width, width), F32)
    for k in range(width // groups):
        picked = jnp.sum(jnp.where(lanes == lace_ref[0, k], prod, 0.0), axis=1, keepdims=True)
        on = same & ((col // groups) == k) & ((row % spins) == spin_ref[0, k])
        both = both + jnp.where(on, picked, 0.0)
    real, imag = both[:width], both[width:]
    return jnp.concatenate(
        [jnp.concatenate([real, -imag], 1), jnp.concatenate([imag, real], 1)], 0
    )


def mix_kernel(noise_ref, probe_ref, spin_ref, lace_ref, out_ref):
    out_ref[...] = mixing_matrix(noise_ref, probe_ref, spin_ref, lace_ref, out_ref.shape[0] // 2)


def recombine_kernel(masks, weight_ref, keep_ref, recv_ref, *refs):
    others, out_ref = refs[:-1], refs[-1]
    me = lax.axis_index("tm").astype(jnp.int32)
    total = keep_ref[0] * weight_ref[0, me] + recv_ref[0] * weight_ref[0, me ^ 1]
    for mask, ref in zip(masks, others):
        total += ref[0] * weight_ref[0, me ^ mask] + ref[1] * weight_ref[0, me ^ mask ^ 1]
    out_ref[...] = total


def smear_kernel(high_ref, low_ref, mix_ref, *refs):
    out_ref = refs[-1]
    total = refs[0][...]
    for ref in refs[1:-1]:
        total += ref[...]
    total = dot3(split(mix_ref[...]), split(total))
    width = total.shape[0] // 2
    turned = jnp.concatenate([-total[width:], total[:width]], 0)
    across = ((1,), (1,))
    value = dot3(split(total), (high_ref[0], low_ref[0]), across)
    value += dot3(split(turned), (high_ref[1], low_ref[1]), across)
    out_ref[0, 0] = value[:width]
    out_ref[0, 1] = value[width:]


def per_device(
    evecs,
    solutions,
    sink_time_weight,
    noise_source_vector,
    probe,
    dilution_spin_index,
    dilution_lace_index,
):
    n_time, n_space = lax.axis_size("tm"), lax.axis_size("space")
    rows, modes = evecs.shape[2:]
    width = solutions.shape[3] // n_time
    chips = n_time // 2
    masks = [0] + [2 * m + 1 for m in range(1, chips)]
    keep, send, high, low = project(evecs, solutions, masks)

    def swap(value, mask, space=0):
        pairs = [
            (t * n_space + z, (t ^ mask) * n_space + (z ^ space))
            for t in range(n_time)
            for z in range(n_space)
        ]
        return lax.ppermute(value, ("tm", "space"), pairs)

    recv = swap(send, 1)
    weight = swap(sink_time_weight.T, 1)
    mix = pl.pallas_call(
        mix_kernel,
        in_specs=[VMEM_SPEC, VMEM_SPEC, SMEM_SPEC, SMEM_SPEC],
        out_specs=VMEM_SPEC,
        out_shape=jax.ShapeDtypeStruct((2 * width, 2 * width), F32),
        compiler_params=pltpu.CompilerParams(vmem_limit_bytes=8 << 20),
        name="mix",
    )(noise_source_vector, probe, dilution_spin_index, dilution_lace_index)
    pairs = [jnp.stack([keep[m], recv[m]]) for m in range(1, chips)]
    others = [swap(pair, mask) for pair, mask in zip(pairs, masks[1:])]
    part = pl.pallas_call(
        functools.partial(recombine_kernel, masks[1:]),
        in_specs=[SMEM_SPEC] + [VMEM_SPEC] * (chips + 1),
        out_specs=VMEM_SPEC,
        out_shape=jax.ShapeDtypeStruct((2 * width, modes), F32),
        compiler_params=pltpu.CompilerParams(vmem_limit_bytes=8 << 20),
        name="recombine",
    )(weight, keep[:1], recv[:1], *others)
    parts = [swap(part, 1, mask) for mask in reversed(range(n_space))]
    return pl.pallas_call(
        smear_kernel,
        in_specs=[VMEM_SPEC] * (n_space + 3),
        out_specs=VMEM_SPEC,
        out_shape=jax.ShapeDtypeStruct((1, 2, width, rows), F32),
        compiler_params=pltpu.CompilerParams(vmem_limit_bytes=16 << 20),
        name="smear",
    )(high, low, mix, *parts)


def solution(mesh):
    placed = (
        P("tm", None, "space", None),
        P("tm", None, "space", None),
        P(None, "tm"),
        P("tm", None, None, None),
        P("tm", None, None, None),
        P("tm", None),
        P("tm", None),
    )
    return jax.shard_map(
        per_device,
        mesh=mesh,
        in_specs=placed,
        out_specs=P("tm", None, None, "space"),
        check_vma=False,
    )
```

```python
import functools

import jax
import jax.numpy as jnp
from jax import lax
from jax.experimental import pallas as pl
from jax.experimental.pallas import tpu as pltpu
from jax.sharding import PartitionSpec as P

LACE_CLASSES = 8
STEP = 384
BF16 = jnp.bfloat16
F32 = jnp.float32
VMEM_SPEC = pl.BlockSpec(memory_space=pltpu.VMEM)
SMEM_SPEC = pl.BlockSpec(memory_space=pltpu.SMEM)


def split(x):
    high = x.astype(BF16)
    low = (x - high.astype(F32)).astype(BF16)
    return high, low


def dot3(left, right, contract=((1,), (0,))):
    lh, ll = left
    rh, rl = right
    mul = functools.partial(
        lax.dot_general, dimension_numbers=(contract, ((), ())), preferred_element_type=F32
    )
    rows = lh.shape[0]
    both = mul(jnp.concatenate([lh, ll], 0), rh)
    return both[:rows] + both[rows:] + mul(lh, rl)


def project_kernel(
    masks, evecs_hbm, solutions_hbm, keep_ref, send_ref, high_ref, low_ref, evecs_ref, solutions_ref, total_ref, sems
):
    chunks, _, step, modes = evecs_ref.shape
    cols = solutions_ref.shape[3]
    half = cols // (2 * len(masks))
    copies = []
    for i in range(chunks):
        rows = pl.ds(i * step, step)
        pair = (
            pltpu.make_async_copy(solutions_hbm.at[0, :, rows], solutions_ref.at[i], sems.at[0, i]),
            pltpu.make_async_copy(evecs_hbm.at[0, :, rows], evecs_ref.at[i], sems.at[1, i]),
        )
        for copy in pair:
            copy.start()
        copies.append(pair)
    for i in range(chunks):
        copies[i][0].wait()
        real = solutions_ref[i, 0].T
        imag = solutions_ref[i, 1].T
        left = split(
            jnp.concatenate(
                [jnp.concatenate([real, imag], 0), jnp.concatenate([imag, -real], 0)], 1
            )
        )
        copies[i][1].wait()
        right = split(evecs_ref[i].reshape(2 * step, modes))
        for ref, value in zip((high_ref, low_ref), right):
            for part in range(2):
                ref[part, i * step : (i + 1) * step] = value[part * step : (part + 1) * step]
        value = dot3(left, right)
        if i == 0:
            total_ref[...] = value
        else:
            total_ref[...] += value
    me = lax.axis_index("tm").astype(jnp.int32)
    for out, core in ((keep_ref, 1), (send_ref, 0)):
        for m, mask in enumerate(masks):
            block = me ^ (mask ^ core)
            for part in range(2):
                start = pl.multiple_of(part * cols + block * half, 8)
                out[m, part * half : (part + 1) * half] = total_ref[pl.ds(start, half)]


def project(evecs, solutions, masks):
    chips = len(masks)
    rows, modes = evecs.shape[2:]
    cols = solutions.shape[3]
    block_rows = 2 * cols // (2 * chips)
    step = STEP if rows % STEP == 0 else rows
    chunks = rows // step
    out = jax.ShapeDtypeStruct((chips, block_rows, modes), F32)
    held = jax.ShapeDtypeStruct((2, rows, modes), BF16)
    return pl.pallas_call(
        functools.partial(project_kernel, masks),
        in_specs=[pl.BlockSpec(memory_space=pltpu.HBM)] * 2,
        out_specs=[VMEM_SPEC] * 4,
        scratch_shapes=[
            pltpu.VMEM((chunks, 2, step, modes), F32),
            pltpu.VMEM((chunks, 2, step, cols), F32),
            pltpu.VMEM((2 * cols, modes), F32),
            pltpu.SemaphoreType.DMA((2, chunks)),
        ],
        out_shape=[out, out, held, held],
        compiler_params=pltpu.CompilerParams(vmem_limit_bytes=54_000_000),
        name="project",
    )(evecs, solutions)


def mixing_matrix(noise_ref, probe_ref, spin_ref, lace_ref, width):
    noise_real, noise_imag = noise_ref[0, 0], noise_ref[0, 1]
    probe_real, probe_imag = probe_ref[0, 0], probe_ref[0, 1]
    prod_real = noise_real * probe_real + noise_imag * probe_imag
    prod_imag = noise_real * probe_imag - noise_imag * probe_real
    spins, modes = prod_real.shape
    groups = width // spins
    prod = jnp.concatenate([prod_real] * groups + [prod_imag] * groups, 0)
    lanes = lax.broadcasted_iota(jnp.int32, (2 * width, modes), 1) % LACE_CLASSES
    row = lax.broadcasted_iota(jnp.int32, (2 * width, width), 0) % width
    col = lax.broadcasted_iota(jnp.int32, (2 * width, width), 1)
    same = (row // spins) == (col % groups)
    both = jnp.zeros((2 * width, width), F32)
    for k in range(width // groups):
        picked = jnp.sum(jnp.where(lanes == lace_ref[0, k], prod, 0.0), axis=1, keepdims=True)
        on = same & ((col // groups) == k) & ((row % spins) == spin_ref[0, k])
        both = both + jnp.where(on, picked, 0.0)
    real, imag = both[:width], both[width:]
    return jnp.concatenate(
        [jnp.concatenate([real, -imag], 1), jnp.concatenate([imag, real], 1)], 0
    )


def mix_kernel(masks, noise_ref, probe_ref, spin_ref, lace_ref, weight_ref, out_ref, rows_ref):
    partner = lax.axis_index("tm").astype(jnp.int32) ^ 1
    for i, mask in enumerate(masks):
        for core in range(2):
            value = weight_ref[0, partner ^ mask ^ core]
            rows_ref[2 * i + core : 2 * i + core + 1] = jnp.full((1, rows_ref.shape[1]), value)
    out_ref[...] = mixing_matrix(noise_ref, probe_ref, spin_ref, lace_ref, out_ref.shape[0] // 2)


def recombine_kernel(weight_ref, keep_ref, recv_ref, *refs):
    others, out_ref = refs[:-1], refs[-1]
    total = keep_ref[0] * weight_ref[0:1] + recv_ref[0] * weight_ref[1:2]
    for i, ref in enumerate(others):
        total += ref[0] * weight_ref[2 * i + 2 : 2 * i + 3]
        total += ref[1] * weight_ref[2 * i + 3 : 2 * i + 4]
    out_ref[...] = total


def turn_kernel(high_ref, low_ref, high_out, low_out):
    for part in range(2):
        high_out[part] = high_ref[part].T
        low_out[part] = low_ref[part].T


def smear_kernel(high_ref, low_ref, mix_ref, *refs):
    out_ref = refs[-1]
    total = refs[0][...]
    for ref in refs[1:-1]:
        total += ref[...]
    total = dot3(split(mix_ref[...]), split(total))
    width = total.shape[0] // 2
    turned = jnp.concatenate([-total[width:], total[:width]], 0)
    across = ((1,), (0,))
    value = dot3(split(total), (high_ref[0], low_ref[0]), across)
    value += dot3(split(turned), (high_ref[1], low_ref[1]), across)
    out_ref[0, 0] = value[:width]
    out_ref[0, 1] = value[width:]


def per_device(
    evecs,
    solutions,
    sink_time_weight,
    noise_source_vector,
    probe,
    dilution_spin_index,
    dilution_lace_index,
):
    n_time, n_space = lax.axis_size("tm"), lax.axis_size("space")
    rows, modes = evecs.shape[2:]
    width = solutions.shape[3] // n_time
    chips = n_time // 2
    masks = [0] + [2 * m + 1 for m in range(1, chips)]
    keep, send, high, low = project(evecs, solutions, masks)

    def swap(value, mask, space=0):
        pairs = [
            (t * n_space + z, (t ^ mask) * n_space + (z ^ space))
            for t in range(n_time)
            for z in range(n_space)
        ]
        return lax.ppermute(value, ("tm", "space"), pairs)

    recv = swap(send, 1)
    mix, weight = pl.pallas_call(
        functools.partial(mix_kernel, masks),
        in_specs=[VMEM_SPEC, VMEM_SPEC, SMEM_SPEC, SMEM_SPEC, SMEM_SPEC],
        out_specs=[VMEM_SPEC, VMEM_SPEC],
        out_shape=[
            jax.ShapeDtypeStruct((2 * width, 2 * width), F32),
            jax.ShapeDtypeStruct((n_time, modes), F32),
        ],
        compiler_params=pltpu.CompilerParams(vmem_limit_bytes=8 << 20),
        name="mix",
    )(noise_source_vector, probe, dilution_spin_index, dilution_lace_index, sink_time_weight.T)
    weight = swap(weight, 1)
    turned = jax.ShapeDtypeStruct((2, modes, rows), BF16)
    high, low = pl.pallas_call(
        turn_kernel,
        in_specs=[VMEM_SPEC, VMEM_SPEC],
        out_specs=[VMEM_SPEC, VMEM_SPEC],
        out_shape=[turned, turned],
        compiler_params=pltpu.CompilerParams(vmem_limit_bytes=8 << 20),
        name="turn",
    )(high, low)
    pairs = [jnp.stack([keep[m], recv[m]]) for m in range(1, chips)]
    others = [swap(pair, mask) for pair, mask in zip(pairs, masks[1:])]
    part = pl.pallas_call(
        recombine_kernel,
        in_specs=[VMEM_SPEC] * (chips + 2),
        out_specs=VMEM_SPEC,
        out_shape=jax.ShapeDtypeStruct((2 * width, modes), F32),
        compiler_params=pltpu.CompilerParams(vmem_limit_bytes=8 << 20),
        name="recombine",
    )(weight, keep[:1], recv[:1], *others)
    parts = [swap(part, 1, mask) for mask in reversed(range(n_space))]
    return pl.pallas_call(
        smear_kernel,
        in_specs=[VMEM_SPEC] * (n_space + 3),
        out_specs=VMEM_SPEC,
        out_shape=jax.ShapeDtypeStruct((1, 2, width, rows), F32),
        compiler_params=pltpu.CompilerParams(vmem_limit_bytes=16 << 20),
        name="smear",
    )(high, low, mix, *parts)


def solution(mesh):
    placed = (
        P("tm", None, "space", None),
        P("tm", None, "space", None),
        P(None, "tm"),
        P("tm", None, None, None),
        P("tm", None, None, None),
        P("tm", None),
        P("tm", None),
    )
    return jax.shard_map(
        per_device,
        mesh=mesh,
        in_specs=placed,
        out_specs=P("tm", None, None, "space"),
        check_vma=False,
    )
```

```python
import functools

import jax
import jax.numpy as jnp
from jax import lax
from jax.experimental import pallas as pl
from jax.experimental.pallas import tpu as pltpu
from jax.sharding import PartitionSpec as P

LACE_CLASSES = 8
STEP = 384
BF16 = jnp.bfloat16
F32 = jnp.float32
VMEM_SPEC = pl.BlockSpec(memory_space=pltpu.VMEM)
SMEM_SPEC = pl.BlockSpec(memory_space=pltpu.SMEM)


def split(x):
    high = x.astype(BF16)
    low = (x - high.astype(F32)).astype(BF16)
    return high, low


def dot3(left, right, contract=((1,), (0,))):
    lh, ll = left
    rh, rl = right
    mul = functools.partial(
        lax.dot_general, dimension_numbers=(contract, ((), ())), preferred_element_type=F32
    )
    rows = lh.shape[0]
    both = mul(jnp.concatenate([lh, ll], 0), rh)
    return both[:rows] + both[rows:] + mul(lh, rl)


def project_kernel(
    masks, evecs_hbm, solutions_hbm, send_ref, high_ref, low_ref, keep_high_ref, keep_low_ref,
    evecs_ref, solutions_ref, turned_ref, sems
):
    chunks, _, step, modes = evecs_ref.shape
    cols = solutions_ref.shape[3]
    half = cols // (2 * len(masks))
    copies = []
    for i in range(chunks):
        rows = pl.ds(i * step, step)
        pair = (
            pltpu.make_async_copy(solutions_hbm.at[0, :, rows], solutions_ref.at[i], sems.at[0, i]),
            pltpu.make_async_copy(evecs_hbm.at[0, :, rows], evecs_ref.at[i], sems.at[1, i]),
        )
        for copy in pair:
            copy.start()
        copies.append(pair)
    me = lax.axis_index("tm").astype(jnp.int32)

    def rows_of(core):
        picked = []
        for mask in masks:
            span = pl.ds(pl.multiple_of((me ^ (mask ^ core)) * half, 8), half)
            real, imag = turned_ref[0, span], turned_ref[1, span]
            picked += [jnp.concatenate([real, imag], 1), jnp.concatenate([imag, -real], 1)]
        return split(jnp.concatenate(picked, 0))

    for i in range(chunks):
        copies[i][0].wait()
        for part in range(2):
            turned_ref[part] = solutions_ref[i, part].T
        left = rows_of(0)
        keep_high_ref[i], keep_low_ref[i] = rows_of(1)
        copies[i][1].wait()
        right = split(evecs_ref[i].reshape(2 * step, modes))
        for ref, value in zip((high_ref, low_ref), right):
            ref[i] = value
        value = dot3(left, right).reshape(send_ref.shape)
        if i == 0:
            send_ref[...] = value
        else:
            send_ref[...] += value


def keep_kernel(left_high_ref, left_low_ref, high_ref, low_ref, keep_ref):
    total = None
    for i in range(high_ref.shape[0]):
        value = dot3((left_high_ref[i], left_low_ref[i]), (high_ref[i], low_ref[i]))
        total = value if total is None else total + value
    keep_ref[...] = total.reshape(keep_ref.shape)


def project(evecs, solutions, masks):
    chips = len(masks)
    rows, modes = evecs.shape[2:]
    cols = solutions.shape[3]
    block_rows = 2 * cols // (2 * chips)
    step = STEP if rows % STEP == 0 else rows
    chunks = rows // step
    out = jax.ShapeDtypeStruct((chips, block_rows, modes), F32)
    held = jax.ShapeDtypeStruct((chunks, 2 * step, modes), BF16)
    left = jax.ShapeDtypeStruct((chunks, chips * block_rows, 2 * step), BF16)
    return pl.pallas_call(
        functools.partial(project_kernel, masks),
        in_specs=[pl.BlockSpec(memory_space=pltpu.HBM)] * 2,
        out_specs=[VMEM_SPEC] * 5,
        scratch_shapes=[
            pltpu.VMEM((chunks, 2, step, modes), F32),
            pltpu.VMEM((chunks, 2, step, cols), F32),
            pltpu.VMEM((2, cols, step), F32),
            pltpu.SemaphoreType.DMA((2, chunks)),
        ],
        out_shape=[out, held, held, left, left],
        compiler_params=pltpu.CompilerParams(vmem_limit_bytes=54000000),
        name="project",
    )(evecs, solutions)


def mixing_matrix(noise_ref, probe_ref, spin_ref, lace_ref, width):
    noise_real, noise_imag = noise_ref[0, 0], noise_ref[0, 1]
    probe_real, probe_imag = probe_ref[0, 0], probe_ref[0, 1]
    prod_real = noise_real * probe_real + noise_imag * probe_imag
    prod_imag = noise_real * probe_imag - noise_imag * probe_real
    spins, modes = prod_real.shape
    groups = width // spins
    prod = jnp.concatenate([prod_real] * groups + [prod_imag] * groups, 0)
    lanes = lax.broadcasted_iota(jnp.int32, (2 * width, modes), 1) % LACE_CLASSES
    row = lax.broadcasted_iota(jnp.int32, (2 * width, width), 0) % width
    col = lax.broadcasted_iota(jnp.int32, (2 * width, width), 1)
    same = (row // spins) == (col % groups)
    both = jnp.zeros((2 * width, width), F32)
    for k in range(width // groups):
        picked = jnp.sum(jnp.where(lanes == lace_ref[0, k], prod, 0.0), axis=1, keepdims=True)
        on = same & ((col // groups) == k) & ((row % spins) == spin_ref[0, k])
        both = both + jnp.where(on, picked, 0.0)
    real, imag = both[:width], both[width:]
    return jnp.concatenate(
        [jnp.concatenate([real, -imag], 1), jnp.concatenate([imag, real], 1)], 0
    )


def mix_kernel(masks, noise_ref, probe_ref, spin_ref, lace_ref, weight_ref, out_ref, rows_ref):
    partner = lax.axis_index("tm").astype(jnp.int32) ^ 1
    for i, mask in enumerate(masks):
        for core in range(2):
            value = weight_ref[0, partner ^ mask ^ core]
            rows_ref[2 * i + core : 2 * i + core + 1] = jnp.full((1, rows_ref.shape[1]), value)
    out_ref[...] = mixing_matrix(noise_ref, probe_ref, spin_ref, lace_ref, out_ref.shape[0] // 2)


def recombine_kernel(weight_ref, keep_ref, recv_ref, *refs):
    others, out_ref = refs[:-1], refs[-1]
    total = keep_ref[0] * weight_ref[0:1] + recv_ref[0] * weight_ref[1:2]
    for i, ref in enumerate(others):
        total += ref[0] * weight_ref[2 * i + 2 : 2 * i + 3]
        total += ref[1] * weight_ref[2 * i + 3 : 2 * i + 4]
    out_ref[...] = total


def turn_kernel(high_ref, low_ref, high_out, low_out):
    chunks, rows, _ = high_ref.shape
    step = rows // 2
    for i in range(chunks):
        for part in range(2):
            span = slice(part * step, (part + 1) * step)
            high_out[part, :, i * step : (i + 1) * step] = high_ref[i, span].T
            low_out[part, :, i * step : (i + 1) * step] = low_ref[i, span].T


def smear_kernel(high_ref, low_ref, mix_ref, *refs):
    out_ref = refs[-1]
    total = refs[0][...]
    for ref in refs[1:-1]:
        total += ref[...]
    total = dot3(split(mix_ref[...]), split(total))
    width = total.shape[0] // 2
    turned = jnp.concatenate([-total[width:], total[:width]], 0)
    across = ((1,), (0,))
    value = dot3(split(total), (high_ref[0], low_ref[0]), across)
    value += dot3(split(turned), (high_ref[1], low_ref[1]), across)
    out_ref[0, 0] = value[:width]
    out_ref[0, 1] = value[width:]


def per_device(
    evecs,
    solutions,
    sink_time_weight,
    noise_source_vector,
    probe,
    dilution_spin_index,
    dilution_lace_index,
):
    n_time, n_space = lax.axis_size("tm"), lax.axis_size("space")
    rows, modes = evecs.shape[2:]
    width = solutions.shape[3] // n_time
    chips = n_time // 2
    masks = [0] + [2 * m + 1 for m in range(1, chips)]
    send, high, low, left_high, left_low = project(evecs, solutions, masks)

    def swap(value, mask, space=0):
        pairs = [
            (t * n_space + z, (t ^ mask) * n_space + (z ^ space))
            for t in range(n_time)
            for z in range(n_space)
        ]
        return lax.ppermute(value, ("tm", "space"), pairs)

    recv = swap(send, 1)
    keep = pl.pallas_call(
        keep_kernel,
        in_specs=[VMEM_SPEC] * 4,
        out_specs=VMEM_SPEC,
        out_shape=jax.ShapeDtypeStruct(send.shape, F32),
        compiler_params=pltpu.CompilerParams(vmem_limit_bytes=8 << 20),
        name="keep",
    )(left_high, left_low, high, low)
    mix, weight = pl.pallas_call(
        functools.partial(mix_kernel, masks),
        in_specs=[VMEM_SPEC, VMEM_SPEC, SMEM_SPEC, SMEM_SPEC, SMEM_SPEC],
        out_specs=[VMEM_SPEC, VMEM_SPEC],
        out_shape=[
            jax.ShapeDtypeStruct((2 * width, 2 * width), F32),
            jax.ShapeDtypeStruct((n_time, modes), F32),
        ],
        compiler_params=pltpu.CompilerParams(vmem_limit_bytes=8 << 20),
        name="mix",
    )(noise_source_vector, probe, dilution_spin_index, dilution_lace_index, sink_time_weight.T)
    weight = swap(weight, 1)
    turned = jax.ShapeDtypeStruct((2, modes, rows), BF16)
    high, low = pl.pallas_call(
        turn_kernel,
        in_specs=[VMEM_SPEC, VMEM_SPEC],
        out_specs=[VMEM_SPEC, VMEM_SPEC],
        out_shape=[turned, turned],
        compiler_params=pltpu.CompilerParams(vmem_limit_bytes=8 << 20),
        name="turn",
    )(high, low)
    pairs = [jnp.stack([keep[m], recv[m]]) for m in range(1, chips)]
    others = [swap(pair, mask) for pair, mask in zip(pairs, masks[1:])]
    part = pl.pallas_call(
        recombine_kernel,
        in_specs=[VMEM_SPEC] * (chips + 2),
        out_specs=VMEM_SPEC,
        out_shape=jax.ShapeDtypeStruct((2 * width, modes), F32),
        compiler_params=pltpu.CompilerParams(vmem_limit_bytes=8 << 20),
        name="recombine",
    )(weight, keep[:1], recv[:1], *others)
    parts = [swap(part, 1, mask) for mask in reversed(range(n_space))]
    return pl.pallas_call(
        smear_kernel,
        in_specs=[VMEM_SPEC] * (n_space + 3),
        out_specs=VMEM_SPEC,
        out_shape=jax.ShapeDtypeStruct((1, 2, width, rows), F32),
        compiler_params=pltpu.CompilerParams(vmem_limit_bytes=16 << 20),
        name="smear",
    )(high, low, mix, *parts)


def solution(mesh):
    placed = (
        P("tm", None, "space", None),
        P("tm", None, "space", None),
        P(None, "tm"),
        P("tm", None, None, None),
        P("tm", None, None, None),
        P("tm", None),
        P("tm", None),
    )
    return jax.shard_map(
        per_device,
        mesh=mesh,
        in_specs=placed,
        out_specs=P("tm", None, None, "space"),
        check_vma=False,
    )
```

```python
import functools

import jax
import jax.numpy as jnp
from jax import lax
from jax.experimental import pallas as pl
from jax.experimental.pallas import tpu as pltpu
from jax.sharding import PartitionSpec as P

LACE_CLASSES = 8
STEP = 384
BF16 = jnp.bfloat16
F32 = jnp.float32
VMEM_SPEC = pl.BlockSpec(memory_space=pltpu.VMEM)
SMEM_SPEC = pl.BlockSpec(memory_space=pltpu.SMEM)


def split(x):
    high = x.astype(BF16)
    low = (x - high.astype(F32)).astype(BF16)
    return high, low


def dot3(left, right, contract=((1,), (0,))):
    lh, ll = left
    rh, rl = right
    mul = functools.partial(
        lax.dot_general, dimension_numbers=(contract, ((), ())), preferred_element_type=F32
    )
    rows = lh.shape[0]
    both = mul(jnp.concatenate([lh, ll], 0), rh)
    return both[:rows] + both[rows:] + mul(lh, rl)


def project_kernel(
    masks, evecs_hbm, solutions_hbm, send_ref, high_ref, low_ref, keep_high_ref, keep_low_ref,
    evecs_ref, solutions_ref, turned_ref, left_ref, sems
):
    chunks, _, step, modes = evecs_ref.shape
    cols = solutions_ref.shape[3]
    half = cols // (2 * len(masks))
    copies = []
    for ref, source, sem in ((solutions_ref, solutions_hbm, 0), (evecs_ref, evecs_hbm, 1)):
        for i in range(chunks):
            rows = pl.ds(i * step, step)
            copies.append(pltpu.make_async_copy(source.at[0, :, rows], ref.at[i], sems.at[sem, i]))
            copies[-1].start()
    me = lax.axis_index("tm").astype(jnp.int32)

    def rows_of(core):
        picked = []
        for mask in masks:
            span = pl.ds(pl.multiple_of((me ^ (mask ^ core)) * half, 8), half)
            real, imag = turned_ref[0, span], turned_ref[1, span]
            picked += [jnp.concatenate([real, imag], 1), jnp.concatenate([imag, -real], 1)]
        return split(jnp.concatenate(picked, 0))

    for i in range(chunks):
        copies[i].wait()
        for part in range(2):
            turned_ref[part] = solutions_ref[i, part].T
        left_ref[i, 0], left_ref[i, 1] = rows_of(0)
        keep_high_ref[i], keep_low_ref[i] = rows_of(1)
    for i in range(chunks):
        left = left_ref[i, 0], left_ref[i, 1]
        copies[chunks + i].wait()
        right = split(evecs_ref[i].reshape(2 * step, modes))
        for ref, value in zip((high_ref, low_ref), right):
            ref[i] = value
        value = dot3(left, right).reshape(send_ref.shape)
        if i == 0:
            send_ref[...] = value
        else:
            send_ref[...] += value


def keep_kernel(left_high_ref, left_low_ref, high_ref, low_ref, keep_ref):
    total = None
    for i in range(high_ref.shape[0]):
        value = dot3((left_high_ref[i], left_low_ref[i]), (high_ref[i], low_ref[i]))
        total = value if total is None else total + value
    keep_ref[...] = total.reshape(keep_ref.shape)


def project(evecs, solutions, masks):
    chips = len(masks)
    rows, modes = evecs.shape[2:]
    cols = solutions.shape[3]
    block_rows = 2 * cols // (2 * chips)
    step = STEP if rows % STEP == 0 else rows
    chunks = rows // step
    out = jax.ShapeDtypeStruct((chips, block_rows, modes), F32)
    held = jax.ShapeDtypeStruct((chunks, 2 * step, modes), BF16)
    left = jax.ShapeDtypeStruct((chunks, chips * block_rows, 2 * step), BF16)
    return pl.pallas_call(
        functools.partial(project_kernel, masks),
        in_specs=[pl.BlockSpec(memory_space=pltpu.HBM)] * 2,
        out_specs=[VMEM_SPEC] * 5,
        scratch_shapes=[
            pltpu.VMEM((chunks, 2, step, modes), F32),
            pltpu.VMEM((chunks, 2, step, cols), F32),
            pltpu.VMEM((2, cols, step), F32),
            pltpu.VMEM((chunks, 2, chips * block_rows, 2 * step), BF16),
            pltpu.SemaphoreType.DMA((2, chunks)),
        ],
        out_shape=[out, held, held, left, left],
        compiler_params=pltpu.CompilerParams(vmem_limit_bytes=54000000),
        name="project",
    )(evecs, solutions)


def mixing_matrix(noise_ref, probe_ref, spin_ref, lace_ref, width):
    noise_real, noise_imag = noise_ref[0, 0], noise_ref[0, 1]
    probe_real, probe_imag = probe_ref[0, 0], probe_ref[0, 1]
    prod_real = noise_real * probe_real + noise_imag * probe_imag
    prod_imag = noise_real * probe_imag - noise_imag * probe_real
    spins, modes = prod_real.shape
    groups = width // spins
    prod = jnp.concatenate([prod_real] * groups + [prod_imag] * groups, 0)
    lanes = lax.broadcasted_iota(jnp.int32, (2 * width, modes), 1) % LACE_CLASSES
    row = lax.broadcasted_iota(jnp.int32, (2 * width, width), 0) % width
    col = lax.broadcasted_iota(jnp.int32, (2 * width, width), 1)
    same = (row // spins) == (col % groups)
    both = jnp.zeros((2 * width, width), F32)
    for k in range(width // groups):
        picked = jnp.sum(jnp.where(lanes == lace_ref[0, k], prod, 0.0), axis=1, keepdims=True)
        on = same & ((col // groups) == k) & ((row % spins) == spin_ref[0, k])
        both = both + jnp.where(on, picked, 0.0)
    real, imag = both[:width], both[width:]
    return jnp.concatenate(
        [jnp.concatenate([real, -imag], 1), jnp.concatenate([imag, real], 1)], 0
    )


def mix_kernel(masks, noise_ref, probe_ref, spin_ref, lace_ref, weight_ref, out_ref, rows_ref):
    partner = lax.axis_index("tm").astype(jnp.int32) ^ 1
    for i, mask in enumerate(masks):
        for core in range(2):
            value = weight_ref[0, partner ^ mask ^ core]
            rows_ref[2 * i + core : 2 * i + core + 1] = jnp.full((1, rows_ref.shape[1]), value)
    out_ref[...] = mixing_matrix(noise_ref, probe_ref, spin_ref, lace_ref, out_ref.shape[0] // 2)


def recombine_kernel(weight_ref, keep_ref, recv_ref, *refs):
    others, out_ref = refs[:-1], refs[-1]
    total = keep_ref[0] * weight_ref[0:1] + recv_ref[0] * weight_ref[1:2]
    for i, ref in enumerate(others):
        total += ref[0] * weight_ref[2 * i + 2 : 2 * i + 3]
        total += ref[1] * weight_ref[2 * i + 3 : 2 * i + 4]
    out_ref[...] = total


def turn_kernel(high_ref, low_ref, high_out, low_out):
    chunks, rows, _ = high_ref.shape
    step = rows // 2
    for i in range(chunks):
        for part in range(2):
            span = slice(part * step, (part + 1) * step)
            high_out[part, :, i * step : (i + 1) * step] = high_ref[i, span].T
            low_out[part, :, i * step : (i + 1) * step] = low_ref[i, span].T


def smear_kernel(high_ref, low_ref, mix_ref, *refs):
    out_ref = refs[-1]
    total = refs[0][...]
    for ref in refs[1:-1]:
        total += ref[...]
    total = dot3(split(mix_ref[...]), split(total))
    width = total.shape[0] // 2
    turned = jnp.concatenate([-total[width:], total[:width]], 0)
    across = ((1,), (0,))
    value = dot3(split(total), (high_ref[0], low_ref[0]), across)
    value += dot3(split(turned), (high_ref[1], low_ref[1]), across)
    out_ref[0, 0] = value[:width]
    out_ref[0, 1] = value[width:]


def per_device(
    evecs,
    solutions,
    sink_time_weight,
    noise_source_vector,
    probe,
    dilution_spin_index,
    dilution_lace_index,
):
    n_time, n_space = lax.axis_size("tm"), lax.axis_size("space")
    rows, modes = evecs.shape[2:]
    width = solutions.shape[3] // n_time
    chips = n_time // 2
    masks = [0] + [2 * m + 1 for m in range(1, chips)]
    send, high, low, left_high, left_low = project(evecs, solutions, masks)

    def swap(value, mask, space=0):
        pairs = [
            (t * n_space + z, (t ^ mask) * n_space + (z ^ space))
            for t in range(n_time)
            for z in range(n_space)
        ]
        return lax.ppermute(value, ("tm", "space"), pairs)

    recv = swap(send, 1)
    keep = pl.pallas_call(
        keep_kernel,
        in_specs=[VMEM_SPEC] * 4,
        out_specs=VMEM_SPEC,
        out_shape=jax.ShapeDtypeStruct(send.shape, F32),
        compiler_params=pltpu.CompilerParams(vmem_limit_bytes=8 << 20),
        name="keep",
    )(left_high, left_low, high, low)
    mix, weight = pl.pallas_call(
        functools.partial(mix_kernel, masks),
        in_specs=[VMEM_SPEC, VMEM_SPEC, SMEM_SPEC, SMEM_SPEC, SMEM_SPEC],
        out_specs=[VMEM_SPEC, VMEM_SPEC],
        out_shape=[
            jax.ShapeDtypeStruct((2 * width, 2 * width), F32),
            jax.ShapeDtypeStruct((n_time, modes), F32),
        ],
        compiler_params=pltpu.CompilerParams(vmem_limit_bytes=8 << 20),
        name="mix",
    )(noise_source_vector, probe, dilution_spin_index, dilution_lace_index, sink_time_weight.T)
    weight = swap(weight, 1)
    turned = jax.ShapeDtypeStruct((2, modes, rows), BF16)
    high, low = pl.pallas_call(
        turn_kernel,
        in_specs=[VMEM_SPEC, VMEM_SPEC],
        out_specs=[VMEM_SPEC, VMEM_SPEC],
        out_shape=[turned, turned],
        compiler_params=pltpu.CompilerParams(vmem_limit_bytes=8 << 20),
        name="turn",
    )(high, low)
    pairs = [jnp.stack([keep[m], recv[m]]) for m in range(1, chips)]
    others = [swap(pair, mask) for pair, mask in zip(pairs, masks[1:])]
    part = pl.pallas_call(
        recombine_kernel,
        in_specs=[VMEM_SPEC] * (chips + 2),
        out_specs=VMEM_SPEC,
        out_shape=jax.ShapeDtypeStruct((2 * width, modes), F32),
        compiler_params=pltpu.CompilerParams(vmem_limit_bytes=8 << 20),
        name="recombine",
    )(weight, keep[:1], recv[:1], *others)
    parts = [swap(part, 1, mask) for mask in reversed(range(n_space))]
    return pl.pallas_call(
        smear_kernel,
        in_specs=[VMEM_SPEC] * (n_space + 3),
        out_specs=VMEM_SPEC,
        out_shape=jax.ShapeDtypeStruct((1, 2, width, rows), F32),
        compiler_params=pltpu.CompilerParams(vmem_limit_bytes=16 << 20),
        name="smear",
    )(high, low, mix, *parts)


def solution(mesh):
    placed = (
        P("tm", None, "space", None),
        P("tm", None, "space", None),
        P(None, "tm"),
        P("tm", None, None, None),
        P("tm", None, None, None),
        P("tm", None),
        P("tm", None),
    )
    return jax.shard_map(
        per_device,
        mesh=mesh,
        in_specs=placed,
        out_specs=P("tm", None, None, "space"),
        check_vma=False,
    )
```
